32 devices in a mesh: gx: 4 (over z), gy: 2 (over y), gz: 4 (over x, core).
Axes of the slice: x: 2, y: 2, z: 4, core: 2. Of those that a mesh axis runs over, the one named last changes fastest.
Arguments:
- tokens: bfloat16 [32768, 4096], P(('gx', 'gy', 'gz')), may hold values from -300 to 300
- cotangents: bfloat16 [32768, 1024], P(('gx', 'gy', 'gz')), may hold values from -17 to 17
- master: float32 [4096, 1024], P(('gx', 'gy', 'gz')), may hold values from -0.09375 to 0.09375
- first_moment: float32 [4096, 1024], P(('gx', 'gy', 'gz')), may hold values from -6 to 6
- second_moment: float32 [4096, 1024], P(('gx', 'gy', 'gz')), may hold values from 0.1 to 10
Outputs:
- weights: bfloat16 [4096, 1024], replicated
- new_master: float32 [4096, 1024], P(('gx', 'gy', 'gz'))
- new_first: float32 [4096, 1024], P(('gx', 'gy', 'gz'))
- new_second: float32 [4096, 1024], P(('gx', 'gy', 'gz'))
The draws below stay inside these ranges and needn't reach their ends.
All inputs are finite; a program needn't handle non-finite values.
Results may differ from the reference program's by a relative error of at most 0.002.
Values may be sent and summed in bfloat16 or wider, within the bound.
A program may use at most 128 MiB of HBM per device.

```python
import math
import jax
import jax.numpy as jnp
from jax import lax

D = 4096
PROJ = 1024
TOK_DEV = 1024
ADAM_STEP = 10
REPLICAS = 32
TOKENS = 32768


def draw_tokens(key, part):
    keys = jax.random.split(jax.random.fold_in(key, 11), 8)
    noise = jnp.clip(jax.random.normal(keys[0], (TOKENS, D), jnp.float32), -4.0, 4.0)
    column = jnp.arange(D, dtype=jnp.float32) / D
    jitter = jnp.exp(jax.random.uniform(keys[1], (D,), jnp.float32, 0.0, 1.0))
    owner = jax.random.permutation(keys[2], REPLICAS).astype(jnp.int32)
    device = (jnp.arange(TOKENS, dtype=jnp.int32) // TOK_DEV).astype(jnp.int32)
    block = (jnp.arange(D, dtype=jnp.int32) // (D // REPLICAS)).astype(jnp.int32)
    quiet = jnp.exp(jax.random.uniform(keys[4], (REPLICAS, REPLICAS), jnp.float32, -1.5, 0.0))
    loud_level = 6.0 * jnp.exp(jax.random.uniform(keys[5], (REPLICAS, REPLICAS), jnp.float32, -0.3, 0.0))
    rate = jnp.exp(jax.random.uniform(keys[6], (), jnp.float32, math.log(1.0 / 64.0), math.log(1.0 / 8.0)))
    loud = jax.random.uniform(keys[7], (REPLICAS, REPLICAS), jnp.float32, 0.0, 1.0) < rate
    gain_table = jnp.where(loud, loud_level, quiet)
    gain = gain_table[device[:, None], block[None, :]]
    spiked = jnp.where(block[None, :] == owner[device][:, None], 6.0, gain)
    ramp = 10.0 ** (0.5 * column)
    return (noise * (ramp * jitter)[None, :] * spiked).astype(jnp.bfloat16)


def draw_cotangents(key, part):
    keys = jax.random.split(jax.random.fold_in(key, 23), 2)
    noise = jnp.clip(jax.random.normal(keys[0], (TOKENS, PROJ), jnp.float32), -4.0, 4.0)
    scales = jnp.exp(jax.random.uniform(keys[1], (PROJ,), jnp.float32, -1.2, 1.09))
    return (noise * scales[None, :]).astype(jnp.bfloat16)


def level_of(rng, extent, pieces, least, largest):
    level = 1.0
    for position, parts in pieces:
        heights = jax.random.uniform(jax.random.fold_in(jax.random.fold_in(rng, 6), position), (parts,), jnp.float32, least / len(pieces), largest / len(pieces))
        level = level * jnp.repeat(jnp.exp(heights), extent[position] // parts).reshape((-1,) + (1,) * (len(extent) - 1 - position))
    return level


def scatter_about(own_key, shape, scale, reach, pieces=(), kind=jnp.bfloat16):
    loudness = level_of(own_key, shape, pieces, -0.22, 0.18) if pieces else 1.0
    array = jax.random.normal(own_key, shape, jnp.float32) * scale * loudness
    return jnp.minimum(jnp.maximum(array, -reach), reach).astype(kind)


def setup_inputs(seed: int = 0) -> dict:
    splits = jax.random.split(jax.random.key(seed), 6)
    return {
        "tokens": draw_tokens(jax.random.fold_in(splits[5], 71), 0),
        "cotangents": draw_cotangents(jax.random.fold_in(splits[5], 71), 0),
        "master": scatter_about(splits[2], (D, PROJ), D ** -0.5, 0.09375, ((0, 32),), jnp.float32),
        "first_moment": scatter_about(splits[3], (D, PROJ), 1.0, 6.0, ((0, 32),), jnp.float32),
        "second_moment": jnp.clip(jnp.exp(math.log(10.0) - 4.6051702 * jax.random.uniform(splits[4], (D, PROJ), jnp.float32) ** level_of(splits[4], (D, PROJ), ((0, 32),), -0.2, 0.2)), 0.1, 10.0),
    }


beta_first = 0.9
beta_second = 0.95
learn_rate = 0.001
decay_rate = 0.1
epsilon = 1e-08

def reference(tokens, cotangents, master, first_moment, second_moment):
    gradient = lax.dot_general(tokens, cotangents, (((0,), (0,)), ((), ())), preferred_element_type=jnp.float32)
    squares = jnp.sum(gradient * gradient)
    grad_norm = jnp.sqrt(squares)
    clip_norm = jnp.sqrt(jnp.float32(D * PROJ))
    factor = clip_norm / jnp.maximum(grad_norm, clip_norm)
    clipped = factor * gradient
    new_first = beta_first * first_moment + (1.0 - beta_first) * clipped
    new_second = beta_second * second_moment + (1.0 - beta_second) * clipped * clipped
    first_hat = new_first / (1.0 - beta_first ** ADAM_STEP)
    second_hat = new_second / (1.0 - beta_second ** ADAM_STEP)
    new_master = master - learn_rate * (first_hat / (jnp.sqrt(second_hat) + epsilon) + decay_rate * master)
    weights = new_master.astype(jnp.bfloat16)
    return (weights, new_master, new_first, new_second)
```

```python
import functools
import math

import jax
import jax.numpy as jnp
from jax import lax
from jax.experimental import pallas as pl
from jax.experimental.pallas import tpu as pltpu
from jax.sharding import PartitionSpec as P

ADAM_STEP = 10
beta_first = 0.9
beta_second = 0.95
learn_rate = 0.001
decay_rate = 0.1
epsilon = 1e-08

AXES = ("gx", "gy", "gz")
LANES = 128
MESH = pl.DeviceIdType.MESH


class Copies:
    def __init__(self, send_sem=None, recv_sem=None):
        self.send_sem, self.recv_sem = send_sem, recv_sem
        self.made = []

    def start(self, src, dst, device):
        at = len(self.made)
        copy = pltpu.make_async_remote_copy(
            src_ref=src,
            dst_ref=dst,
            send_sem=self.send_sem.at[at],
            recv_sem=self.recv_sem.at[at],
            device_id=device,
            device_id_type=MESH,
        )
        copy.start()
        self.made.append(copy)
        return copy


def kernel(
    sizes, chunks, clip_norm,
    part, master, first, second,
    weights, new_master, new_first, new_second,
    recv0, send1p, recv1p, send1q, recv1q, send2p, recv2p, send2q, recv2q, send3, recv3,
    grad, squares, full, send_sem, recv_sem, out_sem,
):
    gx, gy, gxx = sizes
    rows = part.shape[4]
    f32, bf16 = jnp.float32, jnp.bfloat16
    z, y, g = lax.axis_index("gx"), lax.axis_index("gy"), lax.axis_index("gz")
    x, core = g // 2, g % 2
    other = 1 - core
    gz = 2 * gxx

    def along_z(o):
        return {"gx": lax.rem(z + o, gx)}

    def along_y(o):
        return {"gy": lax.rem(y + o, gy)}

    def along_x(o):
        return {"gz": lax.rem(x + o, gxx) * 2 + core}

    partner = {"gz": x * 2 + other}

    barrier = pltpu.get_barrier_semaphore()
    for o in range(1, gz):
        pl.semaphore_signal(barrier, inc=1, device_id={"gz": lax.rem(g + o, gz)}, device_id_type=MESH)
    for o in range(1, gy):
        pl.semaphore_signal(barrier, inc=1, device_id=along_y(o), device_id_type=MESH)
    for o in range(1, gx):
        pl.semaphore_signal(barrier, inc=1, device_id=along_z(o), device_id_type=MESH)
    pl.semaphore_wait(barrier, gz + gy + gx - 3)

    copies = Copies(send_sem, recv_sem)
    width = 2 * LANES

    def cols(k):
        return pl.ds(k * width, width)

    def colp(k):
        return pl.ds(k * width, LANES)

    def colq(k):
        return pl.ds(k * width + LANES, LANES)

    lane_p, lane_q = pl.ds(0, LANES), pl.ds(LANES, LANES)

    core_in = [
        copies.start(part.at[:, :, :, other, :, cols(k)], recv0.at[k], partner)
        for k in range(chunks)
    ]

    def pair(k, i, j, l, col, lane):
        return part[i, j, l, core, :, col].astype(f32) + recv0[k, i, j, l, :, lane].astype(f32)

    first_p, first_q, second_p, second_q, third = {}, {}, {}, {}, {}

    def stage1(k):
        core_in[k].wait_recv()
        first_p[k], first_q[k] = [], []
        for o in range(1, gxx):
            xp = lax.rem(x + o, gxx)

            def body(i, _):
                for j in range(gy):
                    send1p[k, o - 1, i, j] = pair(k, i, j, xp, colp(k), lane_p).astype(bf16)
                return 0

            lax.fori_loop(0, gx, body, 0)
            first_p[k].append(copies.start(send1p.at[k, o - 1], recv1p.at[k, o - 1], along_x(o)))
        for o in range(1, gy):
            yp = lax.rem(y + o, gy)

            def body(i, _):
                for l in range(gxx):
                    send1q[k, o - 1, i, l] = pair(k, i, yp, l, colq(k), lane_q).astype(bf16)
                return 0

            lax.fori_loop(0, gx, body, 0)
            first_q[k].append(copies.start(send1q.at[k, o - 1], recv1q.at[k, o - 1], along_y(o)))

    def after_p(k, i, j):
        total = pair(k, i, j, x, colp(k), lane_p)
        for o in range(1, gxx):
            total += recv1p[k, o - 1, i, j].astype(f32)
        return total

    def after_q(k, i, l):
        total = pair(k, i, y, l, colq(k), lane_q)
        for o in range(1, gy):
            total += recv1q[k, o - 1, i, l].astype(f32)
        return total

    def stage2(k):
        second_p[k], second_q[k] = [], []
        for copy in first_p[k]:
            copy.wait_recv()
        for o in range(1, gy):
            yp = lax.rem(y + o, gy)

            def body(i, _):
                send2p[k, o - 1, i] = after_p(k, i, yp).astype(bf16)
                return 0

            lax.fori_loop(0, gx, body, 0)
            second_p[k].append(copies.start(send2p.at[k, o - 1], recv2p.at[k, o - 1], along_y(o)))
        for copy in first_q[k]:
            copy.wait_recv()
        for o in range(1, gxx):
            xp = lax.rem(x + o, gxx)

            def body(i, _):
                send2q[k, o - 1, i] = after_q(k, i, xp).astype(bf16)
                return 0

            lax.fori_loop(0, gx, body, 0)
            second_q[k].append(copies.start(send2q.at[k, o - 1], recv2q.at[k, o - 1], along_x(o)))

    def plane_p(k, i):
        total = after_p(k, i, y)
        for o in range(1, gy):
            total += recv2p[k, o - 1, i].astype(f32)
        return total

    def plane_q(k, i):
        total = after_q(k, i, x)
        for o in range(1, gxx):
            total += recv2q[k, o - 1, i].astype(f32)
        return total

    def stage3(k):
        for copy in second_p[k] + second_q[k]:
            copy.wait_recv()
        third[k] = []
        for o in range(1, gx):
            zp = lax.rem(z + o, gx)
            send3[k, o - 1, :, lane_p] = plane_p(k, zp).astype(bf16)
            send3[k, o - 1, :, lane_q] = plane_q(k, zp).astype(bf16)
            third[k].append(copies.start(send3.at[k, o - 1], recv3.at[k, o - 1], along_z(o)))

    def stage4(k):
        for copy in third[k]:
            copy.wait_recv()
        total = jnp.zeros((8, LANES), f32)
        for lane, col, plane in ((lane_p, colp(k), plane_p), (lane_q, colq(k), plane_q)):
            value = plane(k, z)
            for o in range(1, gx):
                value += recv3[k, o - 1, :, lane].astype(f32)
            grad[:, col] = value
            total += jnp.sum((value * value).reshape(rows // 8, 8, LANES), axis=0)
        return total

    total = jnp.zeros((8, LANES), f32)
    for t in range(chunks + 3):
        if t < chunks:
            stage1(t)
        if 0 <= t - 1 < chunks:
            stage2(t - 1)
        if 0 <= t - 2 < chunks:
            stage3(t - 2)
        if 0 <= t - 3 < chunks:
            total += stage4(t - 3)

    at = 0
    for axis, count in (("gx", gx), ("gy", gy), ("gz", gz)):
        squares[at] = total
        mine = lax.axis_index(axis)
        moved = [
            copies.start(squares.at[at], squares.at[at + o], {axis: lax.rem(mine + o, count)})
            for o in range(1, count)
        ]
        for o, copy in enumerate(moved, 1):
            copy.wait_recv()
            total += squares[at + o]
        at += count
    norm = jnp.sqrt(jnp.broadcast_to(jnp.sum(total, keepdims=True), (8, LANES)))
    factor = (clip_norm / jnp.maximum(norm, clip_norm))[0:1, :]

    fourth = {}

    def update(k):
        for col in (colp(k), colq(k)):
            clipped = factor * grad[:, col]
            m = beta_first * first[:, col] + (1.0 - beta_first) * clipped
            v = beta_second * second[:, col] + (1.0 - beta_second) * clipped * clipped
            new_first[:, col] = m
            new_second[:, col] = v
            first_hat = m / (1.0 - beta_first**ADAM_STEP)
            second_hat = v / (1.0 - beta_second**ADAM_STEP)
            w = master[:, col]
            w = w - learn_rate * (first_hat / (jnp.sqrt(second_hat) + epsilon) + decay_rate * w)
            new_master[:, col] = w
            full[z, y, x, core, :, col] = w.astype(bf16)
        here = full.at[z, y, x, core, :, cols(k)]
        fourth[k] = [copies.start(here, here, along_z(o)) for o in range(1, gx)]

    fifth, sixth, last, stores = {}, {}, {}, []

    def stage5(k):
        for copy in fourth[k]:
            copy.wait_recv()
        p = full.at[:, y, x, core, :, colp(k)]
        q = full.at[:, y, x, core, :, colq(k)]
        fifth[k] = [copies.start(p, p, along_y(o)) for o in range(1, gy)]
        fifth[k] += [copies.start(q, q, along_x(o)) for o in range(1, gxx)]

    def stage6(k):
        for copy in fifth[k]:
            copy.wait_recv()
        p = full.at[:, :, x, core, :, colp(k)]
        q = full.at[:, y, :, core, :, colq(k)]
        sixth[k] = [copies.start(p, p, along_x(o)) for o in range(1, gxx)]
        sixth[k] += [copies.start(q, q, along_y(o)) for o in range(1, gy)]

    def store(k, half, which):
        src = full.at[:, :, :, half, :, cols(k)]
        dst = weights.at[:, :, :, half, :, cols(k)]
        copy = pltpu.make_async_copy(src, dst, out_sem.at[2 * k + which])
        copy.start()
        stores.append(copy)

    def stage7(k):
        for copy in sixth[k]:
            copy.wait_recv()
        half = full.at[:, :, :, core, :, cols(k)]
        last[k] = copies.start(half, half, partner)
        store(k, core, 0)

    def stage8(k):
        last[k].wait_recv()
        store(k, other, 1)

    for k in range(chunks):
        update(k)
    for t in range(chunks + 3):
        if t < chunks:
            stage5(t)
        if 0 <= t - 1 < chunks:
            stage6(t - 1)
        if 0 <= t - 2 < chunks:
            stage7(t - 2)
        if 0 <= t - 3 < chunks:
            stage8(t - 3)
    for copy in copies.made:
        copy.wait_send()
    for copy in stores:
        copy.wait()


def shards(sizes, tokens, cotangents, master, first_moment, second_moment):
    gx, gy, gxx = sizes
    width, columns = tokens.shape[1], cotangents.shape[1]
    rows = master.shape[0]
    chunks = columns // (2 * LANES)
    clip_norm = math.sqrt(width * columns)
    f32, bf16 = jnp.float32, jnp.bfloat16
    partial = lax.dot_general(
        tokens, cotangents, (((0,), (0,)), ((), ())), preferred_element_type=f32
    ).astype(bf16)
    whole = (gx, gy, gxx, 2, rows, columns)
    per_chunk = (1 + 2 * ((gxx - 1) + (gy - 1)) + (gx - 1)) * 2
    count = chunks * per_chunk + gx + gy + 2 * gxx - 3
    block = (rows, LANES)
    vmem = pl.BlockSpec(memory_space=pltpu.VMEM)
    state = jax.ShapeDtypeStruct((rows, columns), f32)

    def twice(*shape):
        return [pltpu.VMEM((chunks,) + shape, bf16)] * 2

    weights, new_master, new_first, new_second = pl.pallas_call(
        functools.partial(kernel, sizes, chunks, clip_norm),
        out_shape=(jax.ShapeDtypeStruct(whole, bf16), state, state, state),
        in_specs=[vmem] * 4,
        out_specs=(pl.BlockSpec(memory_space=pl.ANY), vmem, vmem, vmem),
        scratch_shapes=[
            pltpu.VMEM((chunks, gx, gy, gxx, rows, 2 * LANES), bf16),
            *twice(gxx - 1, gx, gy, *block),
            *twice(gy - 1, gx, gxx, *block),
            *twice(gy - 1, gx, *block),
            *twice(gxx - 1, gx, *block),
            *twice(gx - 1, rows, 2 * LANES),
            pltpu.VMEM((rows, columns), f32),
            pltpu.VMEM((gx + gy + 2 * gxx, 8, LANES), f32),
            pltpu.VMEM(whole, bf16),
            pltpu.SemaphoreType.DMA((count,)),
            pltpu.SemaphoreType.DMA((count,)),
            pltpu.SemaphoreType.DMA((2 * chunks,)),
        ],
        compiler_params=pltpu.CompilerParams(
            collective_id=0, has_side_effects=True, vmem_limit_bytes=48 * 1024 * 1024
        ),
    )(partial.reshape(whole), master, first_moment, second_moment)
    return (weights.reshape(width, columns), new_master, new_first, new_second)


def solution(mesh):
    sizes = (mesh.shape["gx"], mesh.shape["gy"], mesh.shape["gz"] // 2)
    split = P(AXES, None)
    return jax.shard_map(
        functools.partial(shards, sizes),
        mesh=mesh,
        in_specs=(split,) * 5,
        out_specs=(P(), split, split, split),
        check_vma=False,
    )
```

```python
import functools
import math

import jax
import jax.numpy as jnp
from jax import lax
from jax.experimental import pallas as pl
from jax.experimental.pallas import tpu as pltpu
from jax.sharding import PartitionSpec as P

ADAM_STEP = 10
beta_first = 0.9
beta_second = 0.95
learn_rate = 0.001
decay_rate = 0.1
epsilon = 1e-08

AXES = ("gx", "gy", "gz")
LANES = 128
MESH = pl.DeviceIdType.MESH


class Copies:
    def __init__(self, send_sem=None, recv_sem=None):
        self.send_sem, self.recv_sem = send_sem, recv_sem
        self.made = []

    def start(self, src, dst, device):
        at = len(self.made)
        copy = pltpu.make_async_remote_copy(
            src_ref=src,
            dst_ref=dst,
            send_sem=self.send_sem.at[at],
            recv_sem=self.recv_sem.at[at],
            device_id=device,
            device_id_type=MESH,
        )
        copy.start()
        self.made.append(copy)
        return copy


def kernel(
    sizes, chunks, clip_norm,
    tokens, cotangents, master, first, second,
    weights, new_master, new_first, new_second,
    flipped, part, recv0, send1p, recv1p, send1q, recv1q, send2p, recv2p, send2q, recv2q, send3, recv3,
    grad, squares, full, send_sem, recv_sem, out_sem,
):
    gx, gy, gxx = sizes
    rows = part.shape[4]
    f32, bf16 = jnp.float32, jnp.bfloat16
    z, y, g = lax.axis_index("gx"), lax.axis_index("gy"), lax.axis_index("gz")
    x, core = g // 2, g % 2
    other = 1 - core
    gz = 2 * gxx

    def along_z(o):
        return {"gx": lax.rem(z + o, gx)}

    def along_y(o):
        return {"gy": lax.rem(y + o, gy)}

    def along_x(o):
        return {"gz": lax.rem(x + o, gxx) * 2 + core}

    partner = {"gz": x * 2 + other}

    barrier = pltpu.get_barrier_semaphore()
    for o in range(1, gz):
        pl.semaphore_signal(barrier, inc=1, device_id={"gz": lax.rem(g + o, gz)}, device_id_type=MESH)
    for o in range(1, gy):
        pl.semaphore_signal(barrier, inc=1, device_id=along_y(o), device_id_type=MESH)
    for o in range(1, gx):
        pl.semaphore_signal(barrier, inc=1, device_id=along_z(o), device_id_type=MESH)
    pl.semaphore_wait(barrier, gz + gy + gx - 3)

    copies = Copies(send_sem, recv_sem)
    width = 2 * LANES

    def cols(k):
        return pl.ds(k * width, width)

    def colp(k):
        return pl.ds(k * width, LANES)

    def colq(k):
        return pl.ds(k * width + LANES, LANES)

    lane_p, lane_q = pl.ds(0, LANES), pl.ds(LANES, LANES)

    core_in = {}
    span = max(rows, 2 * LANES)

    def stage0(k):
        right = cotangents[:, cols(k)]

        def body(b, _):
            here = pl.ds(pl.multiple_of(b * span, span), span)
            if k == 0:
                left = tokens[:, here].T
                flipped[here, :] = left
            else:
                left = flipped[here, :]
            product = jnp.dot(left, right, preferred_element_type=f32).astype(bf16)
            for e in range(span // rows):
                d = b * (span // rows) + e
                i, j, l = d // (gy * gz), lax.rem(d // gz, gy), lax.rem(d, gz) // 2
                part[i, j, l, lax.rem(d, 2), :, cols(k)] = product[e * rows : (e + 1) * rows]
            return 0

        lax.fori_loop(0, tokens.shape[1] // span, body, 0)
        core_in[k] = copies.start(part.at[:, :, :, other, :, cols(k)], recv0.at[k], partner)

    def pair(k, i, j, l, col, lane):
        return part[i, j, l, core, :, col].astype(f32) + recv0[k, i, j, l, :, lane].astype(f32)

    first_p, first_q, second_p, second_q, third = {}, {}, {}, {}, {}

    def stage1(k):
        core_in[k].wait_recv()
        first_p[k], first_q[k] = [], []
        for o in range(1, gxx):
            xp = lax.rem(x + o, gxx)

            def body(i, _):
                for j in range(gy):
                    send1p[k, o - 1, i, j] = pair(k, i, j, xp, colp(k), lane_p).astype(bf16)
                return 0

            lax.fori_loop(0, gx, body, 0)
            first_p[k].append(copies.start(send1p.at[k, o - 1], recv1p.at[k, o - 1], along_x(o)))
        for o in range(1, gy):
            yp = lax.rem(y + o, gy)

            def body(i, _):
                for l in range(gxx):
                    send1q[k, o - 1, i, l] = pair(k, i, yp, l, colq(k), lane_q).astype(bf16)
                return 0

            lax.fori_loop(0, gx, body, 0)
            first_q[k].append(copies.start(send1q.at[k, o - 1], recv1q.at[k, o - 1], along_y(o)))

    def after_p(k, i, j):
        total = pair(k, i, j, x, colp(k), lane_p)
        for o in range(1, gxx):
            total += recv1p[k, o - 1, i, j].astype(f32)
        return total

    def after_q(k, i, l):
        total = pair(k, i, y, l, colq(k), lane_q)
        for o in range(1, gy):
            total += recv1q[k, o - 1, i, l].astype(f32)
        return total

    def stage2(k):
        second_p[k], second_q[k] = [], []
        for copy in first_p[k]:
            copy.wait_recv()
        for o in range(1, gy):
            yp = lax.rem(y + o, gy)

            def body(i, _):
                send2p[k, o - 1, i] = after_p(k, i, yp).astype(bf16)
                return 0

            lax.fori_loop(0, gx, body, 0)
            second_p[k].append(copies.start(send2p.at[k, o - 1], recv2p.at[k, o - 1], along_y(o)))
        for copy in first_q[k]:
            copy.wait_recv()
        for o in range(1, gxx):
            xp = lax.rem(x + o, gxx)

            def body(i, _):
                send2q[k, o - 1, i] = after_q(k, i, xp).astype(bf16)
                return 0

            lax.fori_loop(0, gx, body, 0)
            second_q[k].append(copies.start(send2q.at[k, o - 1], recv2q.at[k, o - 1], along_x(o)))

    def plane_p(k, i):
        total = after_p(k, i, y)
        for o in range(1, gy):
            total += recv2p[k, o - 1, i].astype(f32)
        return total

    def plane_q(k, i):
        total = after_q(k, i, x)
        for o in range(1, gxx):
            total += recv2q[k, o - 1, i].astype(f32)
        return total

    def stage3(k):
        for copy in second_p[k] + second_q[k]:
            copy.wait_recv()
        third[k] = []
        for o in range(1, gx):
            zp = lax.rem(z + o, gx)
            send3[k, o - 1, :, lane_p] = plane_p(k, zp).astype(bf16)
            send3[k, o - 1, :, lane_q] = plane_q(k, zp).astype(bf16)
            third[k].append(copies.start(send3.at[k, o - 1], recv3.at[k, o - 1], along_z(o)))

    def stage4(k):
        for copy in third[k]:
            copy.wait_recv()
        total = jnp.zeros((8, LANES), f32)
        for lane, col, plane in ((lane_p, colp(k), plane_p), (lane_q, colq(k), plane_q)):
            value = plane(k, z)
            for o in range(1, gx):
                value += recv3[k, o - 1, :, lane].astype(f32)
            grad[:, col] = value
            total += jnp.sum((value * value).reshape(rows // 8, 8, LANES), axis=0)
        return total

    total = jnp.zeros((8, LANES), f32)
    stage0(0)
    for t in range(chunks + 3):
        if t + 1 < chunks:
            stage0(t + 1)
        if t < chunks:
            stage1(t)
        if 0 <= t - 1 < chunks:
            stage2(t - 1)
        if 0 <= t - 2 < chunks:
            stage3(t - 2)
        if 0 <= t - 3 < chunks:
            total += stage4(t - 3)

    at = 0
    for axis, count in (("gx", gx), ("gy", gy), ("gz", gz)):
        squares[at] = total
        mine = lax.axis_index(axis)
        moved = [
            copies.start(squares.at[at], squares.at[at + o], {axis: lax.rem(mine + o, count)})
            for o in range(1, count)
        ]
        for o, copy in enumerate(moved, 1):
            copy.wait_recv()
            total += squares[at + o]
        at += count
    norm = jnp.sqrt(jnp.broadcast_to(jnp.sum(total, keepdims=True), (8, LANES)))
    factor = (clip_norm / jnp.maximum(norm, clip_norm))[0:1, :]

    fourth = {}

    def update(k):
        for col in (colp(k), colq(k)):
            clipped = factor * grad[:, col]
            m = beta_first * first[:, col] + (1.0 - beta_first) * clipped
            v = beta_second * second[:, col] + (1.0 - beta_second) * clipped * clipped
            new_first[:, col] = m
            new_second[:, col] = v
            first_hat = m / (1.0 - beta_first**ADAM_STEP)
            second_hat = v / (1.0 - beta_second**ADAM_STEP)
            w = master[:, col]
            w = w - learn_rate * (first_hat / (jnp.sqrt(second_hat) + epsilon) + decay_rate * w)
            new_master[:, col] = w
            full[z, y, x, core, :, col] = w.astype(bf16)
        here = full.at[z, y, x, core, :, cols(k)]
        fourth[k] = [copies.start(here, here, along_z(o)) for o in range(1, gx)]

    fifth, sixth, last, stores = {}, {}, {}, []

    def stage5(k):
        for copy in fourth[k]:
            copy.wait_recv()
        p = full.at[:, y, x, core, :, colp(k)]
        q = full.at[:, y, x, core, :, colq(k)]
        fifth[k] = [copies.start(p, p, along_y(o)) for o in range(1, gy)]
        fifth[k] += [copies.start(q, q, along_x(o)) for o in range(1, gxx)]

    def stage6(k):
        for copy in fifth[k]:
            copy.wait_recv()
        p = full.at[:, :, x, core, :, colp(k)]
        q = full.at[:, y, :, core, :, colq(k)]
        sixth[k] = [copies.start(p, p, along_x(o)) for o in range(1, gxx)]
        sixth[k] += [copies.start(q, q, along_y(o)) for o in range(1, gy)]

    def store(k, half, which):
        src = full.at[:, :, :, half, :, cols(k)]
        dst = weights.at[:, :, :, half, :, cols(k)]
        copy = pltpu.make_async_copy(src, dst, out_sem.at[2 * k + which])
        copy.start()
        stores.append(copy)

    def stage7(k):
        for copy in sixth[k]:
            copy.wait_recv()
        half = full.at[:, :, :, core, :, cols(k)]
        last[k] = copies.start(half, half, partner)
        store(k, core, 0)

    def stage8(k):
        last[k].wait_recv()
        store(k, other, 1)

    for k in range(chunks):
        update(k)
    for t in range(chunks + 3):
        if t < chunks:
            stage5(t)
        if 0 <= t - 1 < chunks:
            stage6(t - 1)
        if 0 <= t - 2 < chunks:
            stage7(t - 2)
        if 0 <= t - 3 < chunks:
            stage8(t - 3)
    for copy in copies.made:
        copy.wait_send()
    for copy in stores:
        copy.wait()


def shards(sizes, tokens, cotangents, master, first_moment, second_moment):
    gx, gy, gxx = sizes
    width, columns = tokens.shape[1], cotangents.shape[1]
    rows = master.shape[0]
    chunks = columns // (2 * LANES)
    clip_norm = math.sqrt(width * columns)
    f32, bf16 = jnp.float32, jnp.bfloat16
    whole = (gx, gy, gxx, 2, rows, columns)
    per_chunk = (1 + 2 * ((gxx - 1) + (gy - 1)) + (gx - 1)) * 2
    count = chunks * per_chunk + gx + gy + 2 * gxx - 3
    block = (rows, LANES)
    vmem = pl.BlockSpec(memory_space=pltpu.VMEM)
    state = jax.ShapeDtypeStruct((rows, columns), f32)

    def twice(*shape):
        return [pltpu.VMEM((chunks,) + shape, bf16)] * 2

    weights, new_master, new_first, new_second = pl.pallas_call(
        functools.partial(kernel, sizes, chunks, clip_norm),
        out_shape=(jax.ShapeDtypeStruct(whole, bf16), state, state, state),
        in_specs=[vmem] * 5,
        out_specs=(pl.BlockSpec(memory_space=pl.ANY), vmem, vmem, vmem),
        scratch_shapes=[
            pltpu.VMEM((width, tokens.shape[0]), bf16),
            pltpu.VMEM(whole, bf16),
            pltpu.VMEM((chunks, gx, gy, gxx, rows, 2 * LANES), bf16),
            *twice(gxx - 1, gx, gy, *block),
            *twice(gy - 1, gx, gxx, *block),
            *twice(gy - 1, gx, *block),
            *twice(gxx - 1, gx, *block),
            *twice(gx - 1, rows, 2 * LANES),
            pltpu.VMEM((rows, columns), f32),
            pltpu.VMEM((gx + gy + 2 * gxx, 8, LANES), f32),
            pltpu.VMEM(whole, bf16),
            pltpu.SemaphoreType.DMA((count,)),
            pltpu.SemaphoreType.DMA((count,)),
            pltpu.SemaphoreType.DMA((2 * chunks,)),
        ],
        compiler_params=pltpu.CompilerParams(
            collective_id=0, has_side_effects=True, vmem_limit_bytes=56 * 1024 * 1024
        ),
    )(tokens, cotangents, master, first_moment, second_moment)
    return (weights.reshape(width, columns), new_master, new_first, new_second)


def solution(mesh):
    sizes = (mesh.shape["gx"], mesh.shape["gy"], mesh.shape["gz"] // 2)
    split = P(AXES, None)
    return jax.shard_map(
        functools.partial(shards, sizes),
        mesh=mesh,
        in_specs=(split,) * 5,
        out_specs=(P(), split, split, split),
        check_vma=False,
    )
```
